8 devices in a mesh: dp: 1 (over z), sp: 2 (over y), tp: 4 (over x, core).
Axes of the slice: x: 2, y: 2, z: 1, core: 2. Of those that a mesh axis runs over, the one named last changes fastest.
Arguments:
- latents: bfloat16 [1, 256, 1280], P('dp')
- queries: bfloat16 [1, 512, 768], P('dp', 'sp')
- lat_ln1: float32 [1280], replicated
- lat_wq: bfloat16 [1280, 8, 160], P(None, 'tp')
- lat_wk: bfloat16 [1280, 8, 160], P(None, 'tp')
- lat_wv: bfloat16 [1280, 8, 160], P(None, 'tp')
- lat_wo: bfloat16 [8, 160, 1280], P('tp')
- lat_ln2: float32 [1280], replicated
- lat_up: bfloat16 [1280, 1280], P(None, 'tp')
- lat_down: bfloat16 [1280, 1280], P('tp')
- dec_lnq: float32 [768], replicated
- dec_lnkv: float32 [1280], replicated
- dec_wq: bfloat16 [768, 768], replicated
- dec_wk: bfloat16 [1280, 768], replicated
- dec_wv: bfloat16 [1280, 768], replicated
- dec_wo: bfloat16 [768, 768], replicated
- dec_ln: float32 [768], replicated
- dec_up: bfloat16 [768, 768], replicated
- dec_down: bfloat16 [768, 768], replicated
- dec_out: bfloat16 [768, 32000], replicated
Outputs:
- output: bfloat16 [1, 512, 32000], P('dp', 'sp')
All inputs are finite; a program needn't handle non-finite values.
Results may differ from the reference program's by a relative error of at most 0.0194839.
Values are sent between devices in bfloat16 or wider.
A program may use at most 1 GiB of HBM per device.

```python
import jax
import jax.numpy as jnp
from jax import lax

BATCH = 1
LATENTS = 256
WIDTH = 1280
HEADS = 8
HEAD_DIM = 160
MLP_WIDTH = 1280
QUERY_CH = 768
DEC_WIDTH = 768
OUT_CH = 32000
QUERIES = 512
QUERY_BLOCK = 256
LN_EPS = 1e-5


def layer_norm(rows_in, gain_vec):
    widened = rows_in.astype(jnp.float32)
    row_mean = jnp.mean(widened, axis=-1, keepdims=True)
    row_var = jnp.mean(jnp.square(widened - row_mean), axis=-1, keepdims=True)
    return ((widened - row_mean) * lax.rsqrt(row_var + LN_EPS) * gain_vec).astype(jnp.bfloat16)


def setup_inputs(seed: int = 0, part: int = 0) -> dict:
    shared = jax.random.split(jax.random.key(seed), 18)
    own_keys = jax.random.split(jax.random.fold_in(jax.random.key(seed + 1), part), 2)

    def draw_normal(rng_key, arr_shape, std_scale):
        return (jax.random.normal(rng_key, arr_shape, jnp.float32) * std_scale).astype(jnp.bfloat16)

    def draw_gain(rng_key, vec_len):
        return 1.0 + 0.3 * jax.random.normal(rng_key, (vec_len,), jnp.float32)

    head_shape = (WIDTH, HEADS, HEAD_DIM)
    return {
        "latents": draw_normal(own_keys[0], (BATCH, LATENTS, WIDTH), 1.0),
        "queries": draw_normal(own_keys[1], (BATCH, QUERIES, QUERY_CH), 1.0),
        "lat_ln1": draw_gain(shared[0], WIDTH),
        "lat_wq": draw_normal(shared[1], head_shape, 1.5 * WIDTH ** -0.5),
        "lat_wk": draw_normal(shared[2], head_shape, 1.5 * WIDTH ** -0.5),
        "lat_wv": draw_normal(shared[3], head_shape, WIDTH ** -0.5),
        "lat_wo": draw_normal(shared[4], (HEADS, HEAD_DIM, WIDTH), (HEADS * HEAD_DIM) ** -0.5),
        "lat_ln2": draw_gain(shared[5], WIDTH),
        "lat_up": draw_normal(shared[6], (WIDTH, MLP_WIDTH), WIDTH ** -0.5),
        "lat_down": draw_normal(shared[7], (MLP_WIDTH, WIDTH), MLP_WIDTH ** -0.5),
        "dec_lnq": draw_gain(shared[8], QUERY_CH),
        "dec_lnkv": draw_gain(shared[9], WIDTH),
        "dec_wq": draw_normal(shared[10], (QUERY_CH, DEC_WIDTH), 1.5 * QUERY_CH ** -0.5),
        "dec_wk": draw_normal(shared[11], (WIDTH, DEC_WIDTH), 1.5 * WIDTH ** -0.5),
        "dec_wv": draw_normal(shared[12], (WIDTH, DEC_WIDTH), 2.0 * WIDTH ** -0.5),
        "dec_wo": draw_normal(shared[13], (DEC_WIDTH, DEC_WIDTH), 1.5 * DEC_WIDTH ** -0.5),
        "dec_ln": draw_gain(shared[14], DEC_WIDTH),
        "dec_up": draw_normal(shared[15], (DEC_WIDTH, DEC_WIDTH), DEC_WIDTH ** -0.5),
        "dec_down": draw_normal(shared[16], (DEC_WIDTH, DEC_WIDTH), DEC_WIDTH ** -0.5),
        "dec_out": draw_normal(shared[17], (DEC_WIDTH, OUT_CH), DEC_WIDTH ** -0.5),
    }


def latent_layer(z_one, lat_ln1, lat_wq, lat_wk, lat_wv, lat_wo, lat_ln2, lat_up, lat_down):
    normed = layer_norm(z_one, lat_ln1).astype(jnp.float32)
    q_heads = jnp.einsum("nd,dhe->nhe", normed, lat_wq.astype(jnp.float32)).astype(jnp.bfloat16)
    k_heads = jnp.einsum("nd,dhe->nhe", normed, lat_wk.astype(jnp.float32)).astype(jnp.bfloat16)
    v_heads = jnp.einsum("nd,dhe->nhe", normed, lat_wv.astype(jnp.float32)).astype(jnp.bfloat16)
    scores = jnp.einsum("qhe,khe->hqk", q_heads.astype(jnp.float32), k_heads.astype(jnp.float32)) * HEAD_DIM ** -0.5
    attn_probs = jax.nn.softmax(scores, axis=-1).astype(jnp.bfloat16)
    context = jnp.einsum("hqk,khe->qhe", attn_probs.astype(jnp.float32), v_heads.astype(jnp.float32)).astype(jnp.bfloat16)
    attn_out = jnp.einsum("qhe,hed->qd", context.astype(jnp.float32), lat_wo.astype(jnp.float32))
    z_mid = (z_one.astype(jnp.float32) + attn_out).astype(jnp.bfloat16)
    hidden = jax.nn.gelu(jnp.dot(layer_norm(z_mid, lat_ln2), lat_up, preferred_element_type=jnp.float32), approximate=False).astype(jnp.bfloat16)
    return (z_mid.astype(jnp.float32) + jnp.dot(hidden, lat_down, preferred_element_type=jnp.float32)).astype(jnp.bfloat16)


def decode_block(q_block, all_keys, all_values, dec_lnq, dec_wq, dec_wo, dec_ln, dec_up, dec_down, dec_out):
    q_proj = jnp.dot(layer_norm(q_block, dec_lnq), dec_wq, preferred_element_type=jnp.float32).astype(jnp.bfloat16)
    scores = jnp.dot(q_proj, all_keys.T, preferred_element_type=jnp.float32) * DEC_WIDTH ** -0.5
    attn_probs = jax.nn.softmax(scores, axis=-1).astype(jnp.bfloat16)
    context = jnp.dot(attn_probs, all_values, preferred_element_type=jnp.float32).astype(jnp.bfloat16)
    mixed_rows = (q_proj.astype(jnp.float32) + jnp.dot(context, dec_wo, preferred_element_type=jnp.float32)).astype(jnp.bfloat16)
    hidden = jax.nn.gelu(jnp.dot(layer_norm(mixed_rows, dec_ln), dec_up, preferred_element_type=jnp.float32), approximate=False).astype(jnp.bfloat16)
    final_rows = (mixed_rows.astype(jnp.float32) + jnp.dot(hidden, dec_down, preferred_element_type=jnp.float32)).astype(jnp.bfloat16)
    return jnp.dot(final_rows, dec_out, preferred_element_type=jnp.float32).astype(jnp.bfloat16)


def reference(latents, queries, lat_ln1, lat_wq, lat_wk, lat_wv, lat_wo, lat_ln2, lat_up, lat_down, dec_lnq, dec_lnkv, dec_wq, dec_wk, dec_wv, dec_wo, dec_ln, dec_up, dec_down, dec_out):
    def one_item(item_pair):
        z_one, q_one = item_pair
        z_new = latent_layer(z_one, lat_ln1, lat_wq, lat_wk, lat_wv, lat_wo, lat_ln2, lat_up, lat_down)
        kv_in = layer_norm(z_new, dec_lnkv)
        all_keys = jnp.dot(kv_in, dec_wk, preferred_element_type=jnp.float32).astype(jnp.bfloat16)
        all_values = jnp.dot(kv_in, dec_wv, preferred_element_type=jnp.float32).astype(jnp.bfloat16)
        query_blocks = q_one.reshape(QUERIES // QUERY_BLOCK, QUERY_BLOCK, QUERY_CH)
        out_blocks = lax.map(lambda q_block: decode_block(q_block, all_keys, all_values, dec_lnq, dec_wq, dec_wo, dec_ln, dec_up, dec_down, dec_out), query_blocks)
        return out_blocks.reshape(QUERIES, OUT_CH)
    return lax.map(one_item, (latents, queries))
```

```python
import functools

import jax
import jax.numpy as jnp
from jax import lax
from jax.experimental import pallas as pl
from jax.experimental.pallas import tpu as pltpu
from jax.sharding import PartitionSpec as P

LN_EPS = 1e-5
MESH = pl.DeviceIdType.MESH
BF16 = jnp.bfloat16
F32 = jnp.float32

CHUNKS = 2
PRE_COLS = 28160
BLOCK = 6400


def dot(a, b):
    return lax.dot_general(a, b, (((1,), (0,)), ((), ())), preferred_element_type=F32)


def dot_nt(a, b):
    return lax.dot_general(a, b, (((1,), (1,)), ((), ())), preferred_element_type=F32)


def norm_rows(wide, gain):
    mean = jnp.mean(wide, axis=-1, keepdims=True)
    cent = wide - mean
    var = jnp.mean(cent * cent, axis=-1, keepdims=True)
    return (cent * lax.rsqrt(var + LN_EPS) * gain).astype(BF16)


def gelu(v):
    return 0.5 * v * (1.0 + lax.erf(v * (0.5**0.5)))


def softmax_rows(scores, scale):
    scaled = scores * scale
    top = jnp.max(scaled, axis=-1, keepdims=True)
    expd = jnp.exp(scaled - top)
    return (expd * (1.0 / jnp.sum(expd, axis=-1, keepdims=True))).astype(BF16)


def front_kernel(
    lat_in, qry_in, g1_in, wq_in, wk_in, wv_in, wo_in, g2_in, up_in, down_in,
    gq_in, gkv_in, dwq_in, dwk_in, dwv_in, dwo_in, gd_in, dup_in, ddown_in, out_in,
    pre_out, x2_out,
    z, normed, qry, g1, g2, gq, gkv, gd, wq, wk, wv, wo, up, down, dwq, dwk, dwv, dwo, dup, ddown,
    q_h, k_h, v_h, ctx_mine, ctx_send, ctx_recv,
    part1, recv1, mid, part2, recv2, kv_in, qd, kd, vd, mixed,
    load_sem, pre_sem, send_sem, recv_sem,
):
    s = lax.axis_index("sp")
    t = lax.axis_index("tp")
    c = lax.rem(t, 2)
    partner = {"tp": t + 1 - 2 * c}
    across_x = {"tp": lax.rem(t + 2, 4)}
    across_y = {"sp": 1 - s}

    heads, head_dim = wq.shape[0], wq.shape[1]
    rows = z.shape[0]
    half = rows // 2
    mine = half // 2
    step = mine // CHUNKS
    mlp = down_in.shape[0]

    barrier = pltpu.get_barrier_semaphore()
    for peer in (partner, across_x, across_y):
        pl.semaphore_signal(barrier, inc=1, device_id=peer, device_id_type=MESH)

    loads = {}

    def load(name, src, dst):
        copy = pltpu.make_async_copy(src, dst, load_sem.at[len(loads)])
        copy.start()
        loads[name] = copy

    load("z", lat_in, z)
    load("g1", g1_in, g1)
    load("wk", wk_in, wk)
    load("wq", wq_in, wq)
    load("wv", wv_in, wv)
    load("wo", wo_in, wo.at[pl.ds(0, heads * head_dim)])
    load("qry", qry_in, qry)
    load("gq", gq_in, gq)
    load("g2", g2_in, g2)
    load("gkv", gkv_in, gkv)
    load("gd", gd_in, gd)
    load("up", up_in, up.at[pl.ds(0, mlp)])
    load("down", down_in, down.at[pl.ds(0, mlp)])
    load("dwq", dwq_in, dwq)
    load("dwk", dwk_in, dwk)
    load("dwv", dwv_in, dwv)
    load("dwo", dwo_in, dwo)
    load("dup", dup_in, dup)
    load("ddown", ddown_in, ddown)

    pre_pieces = pre_sem.shape[0]
    pre_rows = pre_out.shape[0] // pre_pieces
    pre = []
    for i in range(pre_pieces):
        band = pl.ds(i * pre_rows, pre_rows)
        copy = pltpu.make_async_copy(out_in.at[band, pl.ds(0, PRE_COLS)], pre_out.at[band], pre_sem.at[i])
        copy.start(priority=1)
        pre.append(copy)

    def send(i, src, dst, peer):
        copy = pltpu.make_async_remote_copy(
            src_ref=src, dst_ref=dst, send_sem=send_sem.at[i], recv_sem=recv_sem.at[i], device_id=peer, device_id_type=MESH
        )
        copy.start()
        return copy

    pl.semaphore_wait(barrier, 3)
    swap_wo = send(0, wo_in, wo.at[pl.ds(heads * head_dim, heads * head_dim)], partner)
    swap_up = send(1, up_in, up.at[pl.ds(mlp, mlp)], partner)
    swap_down = send(2, down_in, down.at[pl.ds(mlp, mlp)], partner)

    loads["z"].wait()
    loads["g1"].wait()
    gain1 = g1[...]
    for r in range(0, rows, 16):
        normed[pl.ds(r, 16), :] = norm_rows(z[pl.ds(r, 16), :].astype(F32), gain1)
    loads["wk"].wait()
    for h in range(heads):
        k_h[h] = dot_nt(normed[...], wk[h]).astype(BF16)
    loads["wq"].wait()
    own_half = normed[pl.ds(pl.multiple_of(s * half, half), half), :]
    for h in range(heads):
        q_h[h] = dot_nt(own_half, wq[h]).astype(BF16)
    loads["wv"].wait()
    for h in range(heads):
        v_h[h] = dot_nt(normed[...], wv[h]).astype(BF16)

    def attend(first, dst):
        for h in range(heads):
            scores = dot_nt(q_h[h, pl.ds(first, mine), :], k_h[h])
            probs = softmax_rows(scores, head_dim**-0.5)
            dst[h, :, pl.ds(0, head_dim)] = dot(probs, v_h[h]).astype(BF16)

    attend(pl.multiple_of((1 - c) * mine, mine), ctx_send)
    swap_ctx = send(3, ctx_send, ctx_recv, partner)
    attend(pl.multiple_of(c * mine, mine), ctx_mine)

    loads["wo"].wait()
    swap_wo.wait()
    swap_ctx.wait()
    first_sends, second_sends, kv_part, kv_y, kv_fwd = [], [], [], [], []
    base = 4
    for k in range(CHUNKS):
        band = pl.ds(k * step, step)
        total = None
        for src, row0 in ((ctx_mine, 0), (ctx_recv, heads * head_dim)):
            for h in range(heads):
                term = dot(src[h, band, pl.ds(0, head_dim)], wo[pl.ds(row0 + h * head_dim, head_dim), :])
                total = term if total is None else total + term
        part1[band, :] = total.astype(BF16)
        first_sends.append(send(base + k, part1.at[band], recv1.at[band], across_x))

    loads["qry"].wait()
    loads["gq"].wait()
    loads["dwq"].wait()
    gain_q = gq[...]
    query_rows = qry.shape[0]
    for r in range(0, query_rows, 16):
        mixed[pl.ds(r, 16), :] = norm_rows(qry[pl.ds(r, 16), :].astype(F32), gain_q)
    qd[...] = dot(mixed[...], dwq[...]).astype(BF16)

    for name in ("g2", "up", "down", "gkv"):
        loads[name].wait()
    swap_up.wait()
    swap_down.wait()
    gain2 = g2[...]
    gain_kv = gkv[...]
    base = 4 + CHUNKS
    row_first = s * half + c * mine
    for k in range(CHUNKS):
        band = pl.ds(k * step, step)
        first_sends[k].wait()
        zrows = z[pl.ds(pl.multiple_of(row_first + k * step, step), step), :].astype(F32)
        mid[band, :] = (zrows + (part1[band, :].astype(F32) + recv1[band, :].astype(F32))).astype(BF16)
        hidden = gelu(dot_nt(norm_rows(mid[band, :].astype(F32), gain2), up[...])).astype(BF16)
        part2[band, :] = dot(hidden, down[...]).astype(BF16)
        second_sends.append(send(base + k, part2.at[band], recv2.at[band], across_x))

    base = 4 + 2 * CHUNKS
    for k in range(CHUNKS):
        band = pl.ds(k * step, step)
        second_sends[k].wait()
        full = mid[band, :].astype(F32) + (part2[band, :].astype(F32) + recv2[band, :].astype(F32))
        kv_in[0, band, :] = norm_rows(full.astype(BF16).astype(F32), gain_kv)
        kv_y.append(send(base + k, kv_in.at[0, band], kv_in.at[2, band], across_y))
        kv_part.append(send(base + CHUNKS + k, kv_in.at[0, band], kv_in.at[1, band], partner))

    loads["dwk"].wait()
    loads["dwv"].wait()
    for k in range(CHUNKS):
        kv_part[k].wait()

    def keys_values(group):
        group_rows = jnp.concatenate([kv_in[2 * group], kv_in[2 * group + 1]], axis=0)
        band = pl.ds(group * half, half)
        kd[band, :] = dot(group_rows, dwk[...]).astype(BF16)
        vd[band, :] = dot(group_rows, dwv[...]).astype(BF16)

    keys_values(0)
    base = 4 + 4 * CHUNKS
    for k in range(CHUNKS):
        band = pl.ds(k * step, step)
        kv_y[k].wait()
        kv_fwd.append(send(base + k, kv_in.at[2, band], kv_in.at[3, band], partner))
    for k in range(CHUNKS):
        kv_fwd[k].wait()
    keys_values(1)

    for name in ("dwo", "gd", "dup", "ddown"):
        loads[name].wait()
    gain_d = gd[...]
    blk = query_rows // 2
    for q in range(2):
        band = pl.ds(q * blk, blk)
        probs = softmax_rows(dot_nt(qd[band, :], kd[...]), qd.shape[1] ** -0.5)
        context = dot(probs, vd[...]).astype(BF16)
        mixed[band, :] = (qd[band, :].astype(F32) + dot(context, dwo[...])).astype(BF16)
    for q in range(2):
        band = pl.ds(q * blk, blk)
        hidden = gelu(dot(norm_rows(mixed[band, :].astype(F32), gain_d), dup[...])).astype(BF16)
        x2_out[band, :] = (mixed[band, :].astype(F32) + dot(hidden, ddown[...])).astype(BF16)

    for copy in pre:
        copy.wait()


def out_kernel(x_ref, pre_ref, rest_hbm, o_ref, rest, stage, rest_sem, out_sem):
    total = o_ref.shape[1]
    pre_cols = pre_ref.shape[1]
    fetch = pltpu.make_async_copy(rest_hbm.at[:, pl.ds(pre_cols, total - pre_cols)], rest, rest_sem)
    fetch.start()
    copies = []
    first = 0
    widths = []
    left = pre_cols
    while left:
        widths.append((min(BLOCK, left), False))
        left -= widths[-1][0]
    left = total - pre_cols
    while left:
        widths.append((min(2560, left), True))
        left -= widths[-1][0]
    for i, (width, from_rest) in enumerate(widths):
        slot = i % 2
        if i >= 2:
            copies[i - 2].wait()
        if from_rest and not widths[i - 1][1]:
            fetch.wait()
        src, off = (rest, first - pre_cols) if from_rest else (pre_ref, first)
        stage[slot, :, pl.ds(0, width)] = dot(x_ref[...], src[:, pl.ds(off, width)]).astype(BF16)
        copy = pltpu.make_async_copy(stage.at[slot, :, pl.ds(0, width)], o_ref.at[:, pl.ds(first, width)], out_sem.at[slot])
        copy.start()
        copies.append(copy)
        first += width
    copies[-2].wait()
    copies[-1].wait()


def solution(mesh):
    head_split = P(None, "tp", None)
    whole_vec = P(None)
    whole_mat = P(None, None)
    in_specs = (P("dp", None, None), P("dp", "sp", None), whole_vec, head_split, head_split, head_split, P("tp", None, None), whole_vec, P(None, "tp"), P("tp", None), whole_vec, whole_vec, whole_mat, whole_mat, whole_mat, whole_mat, whole_vec, whole_mat, whole_mat, whole_mat)

    def local_step(latents, queries, lat_ln1, lat_wq, lat_wk, lat_wv, lat_wo, lat_ln2, lat_up, lat_down, dec_lnq, dec_lnkv, dec_wq, dec_wk, dec_wv, dec_wo, dec_ln, dec_up, dec_down, dec_out):
        rows, width = latents.shape[1:]
        query_rows, query_ch = queries.shape[1:]
        heads, head_dim = lat_wq.shape[1:]
        mlp = lat_up.shape[1]
        dec = dec_wq.shape[1]
        total = dec_out.shape[1]
        half, mine = rows // 2, rows // 4

        def flip(w):
            return jnp.transpose(w, (1, 2, 0))

        args = [
            latents[0], queries[0], lat_ln1[None], flip(lat_wq), flip(lat_wk), flip(lat_wv), lat_wo.reshape(heads * head_dim, width),
            lat_ln2[None], lat_up.T, lat_down, dec_lnq[None], dec_lnkv[None], dec_wq, dec_wk, dec_wv, dec_wo, dec_ln[None], dec_up, dec_down, dec_out,
        ]
        args = [pltpu.with_memory_space_constraint(a, pltpu.HBM) for a in args]

        def vm(*shape, dtype=BF16):
            return pltpu.VMEM(shape, dtype)

        scratch = [
            vm(rows, width), vm(rows, width), vm(query_rows, query_ch),
            vm(1, width, dtype=F32), vm(1, width, dtype=F32), vm(1, query_ch, dtype=F32), vm(1, width, dtype=F32), vm(1, dec, dtype=F32),
            vm(heads, head_dim, width), vm(heads, head_dim, width), vm(heads, head_dim, width),
            vm(2 * heads * head_dim, width), vm(2 * mlp, width), vm(2 * mlp, width),
            vm(query_ch, dec), vm(width, dec), vm(width, dec), vm(dec, dec), vm(dec, dec), vm(dec, dec),
            vm(heads, half, head_dim), vm(heads, rows, head_dim), vm(heads, rows, head_dim),
            vm(heads, mine, 256), vm(heads, mine, 256), vm(heads, mine, 256),
            vm(mine, width), vm(mine, width), vm(mine, width), vm(mine, width), vm(mine, width),
            vm(4, mine, width), vm(query_rows, dec), vm(rows, dec), vm(rows, dec), vm(query_rows, dec),
            pltpu.SemaphoreType.DMA((19,)), pltpu.SemaphoreType.DMA((8,)),
            pltpu.SemaphoreType.DMA((4 + 5 * CHUNKS,)), pltpu.SemaphoreType.DMA((4 + 5 * CHUNKS,)),
        ]
        pre, x2 = pl.pallas_call(
            front_kernel,
            out_shape=(pltpu.VMEM((dec, PRE_COLS), BF16), jax.ShapeDtypeStruct((query_rows, dec), BF16)),
            in_specs=[pl.BlockSpec(memory_space=pltpu.HBM)] * len(args),
            out_specs=(pl.BlockSpec(memory_space=pltpu.VMEM), pl.BlockSpec(memory_space=pltpu.VMEM)),
            scratch_shapes=scratch,
            compiler_params=pltpu.CompilerParams(collective_id=0, has_side_effects=True, vmem_limit_bytes=22 << 20),
            name="front",
        )(*args)
        out = pl.pallas_call(
            out_kernel,
            out_shape=jax.ShapeDtypeStruct((query_rows, total), BF16),
            in_specs=[pl.BlockSpec(memory_space=pltpu.VMEM), pl.BlockSpec(memory_space=pltpu.VMEM), pl.BlockSpec(memory_space=pltpu.HBM)],
            out_specs=pl.BlockSpec(memory_space=pltpu.HBM),
            scratch_shapes=[vm(dec, total - PRE_COLS), vm(2, query_rows, BLOCK), pltpu.SemaphoreType.DMA, pltpu.SemaphoreType.DMA((2,))],
            compiler_params=pltpu.CompilerParams(vmem_limit_bytes=18 << 20),
            name="project",
        )(x2, pltpu.with_memory_space_constraint(pre, pltpu.VMEM), pltpu.with_memory_space_constraint(dec_out, pltpu.HBM))
        return out[None]

    return jax.shard_map(local_step, mesh=mesh, in_specs=in_specs, out_specs=P("dp", "sp", None), check_vma=False)
```

```python
import functools

import jax
import jax.numpy as jnp
from jax import lax
from jax.experimental import pallas as pl
from jax.experimental.pallas import tpu as pltpu
from jax.sharding import PartitionSpec as P

LN_EPS = 1e-5
MESH = pl.DeviceIdType.MESH
BF16 = jnp.bfloat16
F32 = jnp.float32

CHUNK_ROWS = (32, 16, 16)
CHUNKS = len(CHUNK_ROWS)
PRE_COLS = 26624
TILE = 256
TRIP = 4 * TILE
SLOTS = 6


def dot(a, b):
    return lax.dot_general(a, b, (((1,), (0,)), ((), ())), preferred_element_type=F32)


def dot_nt(a, b):
    return lax.dot_general(a, b, (((1,), (1,)), ((), ())), preferred_element_type=F32)


def norm_rows(wide, gain):
    mean = jnp.mean(wide, axis=-1, keepdims=True)
    cent = wide - mean
    var = jnp.mean(cent * cent, axis=-1, keepdims=True)
    return (cent * lax.rsqrt(var + LN_EPS) * gain).astype(BF16)


def gelu(v):
    return 0.5 * v * (1.0 + lax.erf(v * (0.5**0.5)))


def softmax_rows(scores, scale):
    scaled = scores * scale
    top = jnp.max(scaled, axis=-1, keepdims=True)
    expd = jnp.exp(scaled - top)
    return (expd * (1.0 / jnp.sum(expd, axis=-1, keepdims=True))).astype(BF16)


def front_kernel(
    lat_in, qry_in, g1_in, wq_in, wk_in, wv_in, wo_in, g2_in, up_in, down_in,
    gq_in, gkv_in, dwq_in, dwk_in, dwv_in, dwo_in, gd_in, dup_in, ddown_in, out_in,
    pre_out,
    z, normed, qry, g1, g2, gq, gkv, gd, wq, wk, wv, wo, up, down, dwq, dwk, dwv, dwo, dup, ddown,
    q_h, k_h, v_h, ctx_mine, ctx_send, ctx_recv,
    part1, recv1, mid, part2, recv2, kv_in, qd, kd, vd, mixed,
    load_sem, pre_sem, send_sem, recv_sem,
):
    s = lax.axis_index("sp")
    t = lax.axis_index("tp")
    c = lax.rem(t, 2)
    partner = {"tp": t + 1 - 2 * c}
    across_x = {"tp": lax.rem(t + 2, 4)}
    across_y = {"sp": 1 - s}

    heads, head_dim = wq.shape[0], wq.shape[1]
    rows = z.shape[0]
    half = rows // 2
    mine = half // 2
    starts = [sum(CHUNK_ROWS[:k]) for k in range(CHUNKS)]
    mlp = down_in.shape[0]

    barrier = pltpu.get_barrier_semaphore()
    for peer in (partner, across_x, across_y):
        pl.semaphore_signal(barrier, inc=1, device_id=peer, device_id_type=MESH)

    loads = {}

    def load(name, src, dst):
        copy = pltpu.make_async_copy(src, dst, load_sem.at[len(loads)])
        copy.start()
        loads[name] = copy

    load("z", lat_in, z)
    load("g1", g1_in, g1)
    load("wk", wk_in, wk)
    load("wq", wq_in, wq)
    load("wv", wv_in, wv)
    load("wo", wo_in, wo.at[pl.ds(0, heads * head_dim)])
    load("qry", qry_in, qry)
    load("gq", gq_in, gq)
    load("g2", g2_in, g2)
    load("gkv", gkv_in, gkv)
    load("gd", gd_in, gd)
    load("up", up_in, up.at[pl.ds(0, mlp)])
    load("down", down_in, down.at[pl.ds(0, mlp)])
    load("dwq", dwq_in, dwq)
    load("dwk", dwk_in, dwk)
    load("dwv", dwv_in, dwv)
    load("dwo", dwo_in, dwo)
    load("dup", dup_in, dup)
    load("ddown", ddown_in, ddown)

    pre_pieces = pre_sem.shape[0]
    pre_rows = pre_out.shape[0] // pre_pieces
    pre = []
    for i in range(pre_pieces):
        band = pl.ds(i * pre_rows, pre_rows)
        copy = pltpu.make_async_copy(out_in.at[band, pl.ds(0, PRE_COLS)], pre_out.at[band, pl.ds(0, PRE_COLS)], pre_sem.at[i])
        copy.start(priority=1)
        pre.append(copy)

    def send(i, src, dst, peer):
        copy = pltpu.make_async_remote_copy(
            src_ref=src, dst_ref=dst, send_sem=send_sem.at[i], recv_sem=recv_sem.at[i], device_id=peer, device_id_type=MESH
        )
        copy.start()
        return copy

    loads["z"].wait()
    loads["g1"].wait()
    gain1 = g1[...][None, :]
    for r in range(0, rows, 16):
        normed[pl.ds(r, 16), :] = norm_rows(z[pl.ds(r, 16), :].astype(F32), gain1)
    pl.semaphore_wait(barrier, 3)
    swap_wo = send(0, wo_in, wo.at[pl.ds(heads * head_dim, heads * head_dim)], partner)
    loads["wk"].wait()
    for h in range(heads):
        k_h[h] = dot_nt(normed[...], wk[h]).astype(BF16)
    loads["wq"].wait()
    own_half = normed[pl.ds(pl.multiple_of(s * half, half), half), :]
    for h in range(heads):
        q_h[h] = dot_nt(own_half, wq[h]).astype(BF16)
    loads["wv"].wait()
    for h in range(heads):
        v_h[h] = dot_nt(normed[...], wv[h]).astype(BF16)

    def attend(first, dst):
        for h in range(heads):
            scores = dot_nt(q_h[h, pl.ds(first, mine), :], k_h[h])
            probs = softmax_rows(scores, head_dim**-0.5)
            dst[h, :, pl.ds(0, head_dim)] = dot(probs, v_h[h]).astype(BF16)

    attend(pl.multiple_of((1 - c) * mine, mine), ctx_send)
    swap_ctx = send(3, ctx_send, ctx_recv, partner)
    swap_up = send(1, up_in, up.at[pl.ds(mlp, mlp)], partner)
    swap_down = send(2, down_in, down.at[pl.ds(mlp, mlp)], partner)
    attend(pl.multiple_of(c * mine, mine), ctx_mine)

    loads["wo"].wait()
    swap_wo.wait()
    swap_ctx.wait()
    first_sends, second_sends, kv_part, kv_y, kv_fwd = [], [], [], [], []
    base = 4
    for k in range(CHUNKS):
        band = pl.ds(starts[k], CHUNK_ROWS[k])
        total = None
        for src, row0 in ((ctx_mine, 0), (ctx_recv, heads * head_dim)):
            for h in range(heads):
                term = dot(src[h, band, pl.ds(0, head_dim)], wo[pl.ds(row0 + h * head_dim, head_dim), :])
                total = term if total is None else total + term
        part1[band, :] = total.astype(BF16)
        first_sends.append(send(base + k, part1.at[band], recv1.at[band], across_x))

    loads["qry"].wait()
    loads["gq"].wait()
    loads["dwq"].wait()
    gain_q = gq[...][None, :]
    query_rows = qry.shape[0]
    for r in range(0, query_rows, 16):
        mixed[pl.ds(r, 16), :] = norm_rows(qry[pl.ds(r, 16), :].astype(F32), gain_q)
    qd[...] = dot(mixed[...], dwq[...]).astype(BF16)

    for name in ("g2", "up", "down", "gkv"):
        loads[name].wait()
    swap_up.wait()
    swap_down.wait()
    gain2 = g2[...][None, :]
    gain_kv = gkv[...][None, :]
    base = 4 + CHUNKS
    row_first = s * half + c * mine
    for k in range(CHUNKS):
        band = pl.ds(starts[k], CHUNK_ROWS[k])
        first_sends[k].wait()
        zrows = z[pl.ds(pl.multiple_of(row_first + starts[k], 16), CHUNK_ROWS[k]), :].astype(F32)
        mid[band, :] = (zrows + (part1[band, :].astype(F32) + recv1[band, :].astype(F32))).astype(BF16)
        hidden = gelu(dot_nt(norm_rows(mid[band, :].astype(F32), gain2), up[...])).astype(BF16)
        part2[band, :] = dot(hidden, down[...]).astype(BF16)
        second_sends.append(send(base + k, part2.at[band], recv2.at[band], across_x))

    base = 4 + 2 * CHUNKS
    for k in range(CHUNKS):
        band = pl.ds(starts[k], CHUNK_ROWS[k])
        second_sends[k].wait()
        full = mid[band, :].astype(F32) + (part2[band, :].astype(F32) + recv2[band, :].astype(F32))
        kv_in[0, band, :] = norm_rows(full.astype(BF16).astype(F32), gain_kv)
        kv_y.append(send(base + k, kv_in.at[0, band], kv_in.at[2, band], across_y))
        kv_part.append(send(base + CHUNKS + k, kv_in.at[0, band], kv_in.at[1, band], partner))

    loads["dwk"].wait()
    loads["dwv"].wait()
    for k in range(CHUNKS):
        kv_part[k].wait()

    def keys_values(group):
        group_rows = jnp.concatenate([kv_in[2 * group], kv_in[2 * group + 1]], axis=0)
        band = pl.ds(group * half, half)
        kd[band, :] = dot(group_rows, dwk[...]).astype(BF16)
        vd[band, :] = dot(group_rows, dwv[...]).astype(BF16)

    keys_values(0)
    base = 4 + 4 * CHUNKS
    for k in range(CHUNKS):
        band = pl.ds(starts[k], CHUNK_ROWS[k])
        kv_y[k].wait()
        kv_fwd.append(send(base + k, kv_in.at[2, band], kv_in.at[3, band], partner))
    for k in range(CHUNKS):
        kv_fwd[k].wait()
    keys_values(1)

    for name in ("dwo", "gd", "dup", "ddown"):
        loads[name].wait()
    gain_d = gd[...][None, :]
    blk = query_rows // 2
    for q in range(2):
        band = pl.ds(q * blk, blk)
        probs = softmax_rows(dot_nt(qd[band, :], kd[...]), qd.shape[1] ** -0.5)
        context = dot(probs, vd[...]).astype(BF16)
        mixed[band, :] = (qd[band, :].astype(F32) + dot(context, dwo[...])).astype(BF16)
    for q in range(2):
        band = pl.ds(q * blk, blk)
        hidden = gelu(dot(norm_rows(mixed[band, :].astype(F32), gain_d), dup[...])).astype(BF16)
        pre_out[band, pl.ds(PRE_COLS, qd.shape[1])] = (mixed[band, :].astype(F32) + dot(hidden, ddown[...])).astype(BF16)

    for copy in pre:
        copy.wait()


def out_kernel(pre_ref, rest_hbm, o_ref, rest, stage, rest_sem, out_sem):
    rows = o_ref.shape[0]
    depth = pre_ref.shape[0]
    passes = depth // TILE
    x_col = PRE_COLS
    fetch = pltpu.make_async_copy(rest_hbm.at[:, pl.ds(PRE_COLS, rest.shape[1])], rest, rest_sem)
    fetch.start()
    trips = o_ref.shape[1] // TRIP
    pre_trips = PRE_COLS // TRIP
    slots = stage.shape[0]

    def lhs(k, row0=0, count=rows):
        return pre_ref[pl.ds(row0, count), pl.ds(x_col + k * TILE, TILE)]

    def body(accs, small):
        def push(src, col, k, reg, apart=TILE):
            for q in range(2):
                cols = pl.ds(pl.multiple_of(col + q * apart, TILE), TILE)
                pltpu.matmul_push_rhs(src[pl.ds(k * TILE, TILE), cols], staging_register=reg, mxu_index=q)

        def out_copy(trip, slot):
            cols = pl.ds(pl.multiple_of(trip * TRIP - TRIP // 2, TRIP // 2), TRIP)
            return pltpu.make_async_copy(stage.at[slot], o_ref.at[:, cols], out_sem.at[slot])

        def pop(acc_pair, slot, part):
            for q in range(2):
                stage[slot, :, pl.ds((2 * part + q) * TILE, TILE)] = pltpu.matmul_pop(acc_pair[q]).astype(BF16)

        def one_trip(src, col, slot, next_src, next_col, apart=TILE):
            reg = 0
            for pair in range(2):
                for k in range(passes):
                    for q in range(2):
                        pltpu.matmul_acc_lhs(accs[pair][q], lhs(k), load_staged_rhs=reg)
                    reg = 1 - reg
                    if k + 1 < passes:
                        push(src, col + pair * 2 * TILE, k + 1, reg)
                    elif pair == 0:
                        push(src, col + 2 * TILE, 0, reg)
                    else:
                        push(next_src, next_col, 0, reg, apart)
                    if k == 0:
                        pop(accs[1 - pair], slot, pair)

        def trip_at(i, src, col, next_src, next_col, wait, apart=TILE):
            slot = lax.rem(i, slots)
            if wait:
                out_copy(i - slots, slot).wait()
            one_trip(src, col, slot, next_src, next_col, apart)
            out_copy(i, slot).start()

        for pair in accs:
            for acc in pair:
                pltpu.matmul_pop(acc)
        for acc in small:
            pltpu.matmul_pop(acc)

        push(pre_ref, 0, 0, 0)
        one_trip(pre_ref, 0, 0, pre_ref, TRIP)
        head = pltpu.make_async_copy(stage.at[0, :, pl.ds(TRIP // 2, TRIP // 2)], o_ref.at[:, pl.ds(0, TRIP // 2)], out_sem.at[0])
        head.start()

        def early(i, carry):
            trip_at(i, pre_ref, i * TRIP, pre_ref, (i + 1) * TRIP, False)
            return carry

        def late(i, carry):
            trip_at(i, pre_ref, i * TRIP, pre_ref, (i + 1) * TRIP, True)
            return carry

        def tail(i, carry):
            col = (i - pre_trips) * TRIP
            trip_at(i, rest, col, rest, col + TRIP, True)
            return carry

        lax.fori_loop(1, slots, early, 0)
        head.wait()
        trip_at(slots, pre_ref, slots * TRIP, pre_ref, (slots + 1) * TRIP, False)
        lax.fori_loop(slots + 1, pre_trips - 1, late, 0)
        fetch.wait()
        last = pre_trips - 1
        trip_at(last, pre_ref, last * TRIP, rest, 0, True)
        lax.fori_loop(pre_trips, trips - 1, tail, 0)

        slot = trips % slots
        col = trips * TRIP - PRE_COLS
        trip_at(trips - 1, rest, col - TRIP, rest, col, True, 0)
        half = rows // 2
        out_copy(trips - slots, slot).wait()
        reg = 0
        for k in range(passes):
            for q in range(2):
                pltpu.matmul_acc_lhs(small[q], lhs(k, q * half, half), load_staged_rhs=reg)
            reg = 1 - reg
            if k + 1 < passes:
                push(rest, col, k + 1, reg, 0)
            if k == 0:
                pop(accs[1], slot, 0)
                near = pltpu.make_async_copy(stage.at[slot, :, pl.ds(0, TRIP // 2)], o_ref.at[:, pl.ds(trips * TRIP - TRIP // 2, TRIP // 2)], out_sem.at[slot])
                near.start()
        for q in range(2):
            stage[slot, pl.ds(q * half, half), pl.ds(TRIP // 2, TILE)] = pltpu.matmul_pop(small[q]).astype(BF16)
        end = pltpu.make_async_copy(stage.at[slot, :, pl.ds(TRIP // 2, TILE)], o_ref.at[:, pl.ds(trips * TRIP, TILE)], out_sem.at[slots])
        end.start()
        for i in range(trips - slots + 1, trips):
            out_copy(i, i % slots).wait()
        near.wait()
        end.wait()

    acc = [[pltpu.ACC(q)((rows, TILE), F32) for q in range(2)] for _ in range(2)]
    pl.run_scoped(body, acc, [pltpu.ACC(q)((rows // 2, TILE), F32) for q in range(2)])


def solution(mesh):
    head_split = P(None, "tp", None)
    whole_vec = P(None)
    whole_mat = P(None, None)
    in_specs = (P("dp", None, None), P("dp", "sp", None), whole_vec, head_split, head_split, head_split, P("tp", None, None), whole_vec, P(None, "tp"), P("tp", None), whole_vec, whole_vec, whole_mat, whole_mat, whole_mat, whole_mat, whole_vec, whole_mat, whole_mat, whole_mat)

    def local_step(latents, queries, lat_ln1, lat_wq, lat_wk, lat_wv, lat_wo, lat_ln2, lat_up, lat_down, dec_lnq, dec_lnkv, dec_wq, dec_wk, dec_wv, dec_wo, dec_ln, dec_up, dec_down, dec_out):
        rows, width = latents.shape[1:]
        query_rows, query_ch = queries.shape[1:]
        heads, head_dim = lat_wq.shape[1:]
        mlp = lat_up.shape[1]
        dec = dec_wq.shape[1]
        total = dec_out.shape[1]
        half, mine = rows // 2, rows // 4

        def flip(w):
            return jnp.transpose(w, (1, 2, 0))

        args = [
            latents[0], queries[0], lat_ln1, flip(lat_wq), flip(lat_wk), flip(lat_wv), lat_wo.reshape(heads * head_dim, width),
            lat_ln2, lat_up.T, lat_down, dec_lnq, dec_lnkv, dec_wq, dec_wk, dec_wv, dec_wo, dec_ln, dec_up, dec_down, dec_out,
        ]
        args = [pltpu.with_memory_space_constraint(a, pltpu.HBM) for a in args]

        def vm(*shape, dtype=BF16):
            return pltpu.VMEM(shape, dtype)

        scratch = [
            vm(rows, width), vm(rows, width), vm(query_rows, query_ch),
            vm(width, dtype=F32), vm(width, dtype=F32), vm(query_ch, dtype=F32), vm(width, dtype=F32), vm(dec, dtype=F32),
            vm(heads, head_dim, width), vm(heads, head_dim, width), vm(heads, head_dim, width),
            vm(2 * heads * head_dim, width), vm(2 * mlp, width), vm(2 * mlp, width),
            vm(query_ch, dec), vm(width, dec), vm(width, dec), vm(dec, dec), vm(dec, dec), vm(dec, dec),
            vm(heads, half, head_dim), vm(heads, rows, head_dim), vm(heads, rows, head_dim),
            vm(heads, mine, 256), vm(heads, mine, 256), vm(heads, mine, 256),
            vm(mine, width), vm(mine, width), vm(mine, width), vm(mine, width), vm(mine, width),
            vm(4, mine, width), vm(query_rows, dec), vm(rows, dec), vm(rows, dec), vm(query_rows, dec),
            pltpu.SemaphoreType.DMA((19,)), pltpu.SemaphoreType.DMA((8,)),
            pltpu.SemaphoreType.DMA((4 + 5 * CHUNKS,)), pltpu.SemaphoreType.DMA((4 + 5 * CHUNKS,)),
        ]
        pre = pl.pallas_call(
            front_kernel,
            out_shape=pltpu.VMEM((dec, PRE_COLS + dec), BF16),
            in_specs=[pl.BlockSpec(memory_space=pltpu.HBM)] * len(args),
            out_specs=pl.BlockSpec(memory_space=pltpu.VMEM),
            scratch_shapes=scratch,
            compiler_params=pltpu.CompilerParams(collective_id=0, has_side_effects=True, vmem_limit_bytes=22 << 20),
            name="front",
        )(*args)
        out = pl.pallas_call(
            out_kernel,
            out_shape=jax.ShapeDtypeStruct((query_rows, total), BF16),
            in_specs=[pl.BlockSpec(memory_space=pltpu.VMEM), pl.BlockSpec(memory_space=pltpu.HBM)],
            out_specs=pl.BlockSpec(memory_space=pltpu.HBM),
            scratch_shapes=[vm(dec, total - PRE_COLS), vm(SLOTS, query_rows, TRIP), pltpu.SemaphoreType.DMA, pltpu.SemaphoreType.DMA((SLOTS + 1,))],
            compiler_params=pltpu.CompilerParams(vmem_limit_bytes=18 << 20),
            name="project",
        )(pltpu.with_memory_space_constraint(pre, pltpu.VMEM), pltpu.with_memory_space_constraint(dec_out, pltpu.HBM))
        return out[None]

    return jax.shard_map(local_step, mesh=mesh, in_specs=in_specs, out_specs=P("dp", "sp", None), check_vma=False)
```
